128 devices in a mesh: gene: 16 (over z, x), cell: 8 (over y, core).
Axes of the slice: x: 4, y: 4, z: 4, core: 2. Of those that a mesh axis runs over, the one named last changes fastest.
Arguments:
- counts: bfloat16 [32768, 16384], P('gene', 'cell'), may hold values from -6 to 6
- loadings: float32 [32768, 128], P('gene'), may hold values from -0.03125 to 0.03125
- values: float32 [128], replicated, may hold values from 0.5 to 2
- test_matrix: bfloat16 [16384, 128], P('cell'), may hold values from -0.046875 to 0.046875
- tile_mask: int32 [128, 128], P('gene', 'cell'), may hold values 0 or 1
Outputs:
- new_loadings: float32 [32768, 128], P('gene')
- new_values: float32 [128], replicated
The draws below stay inside these ranges and needn't reach their ends.
All inputs are finite; a program needn't handle non-finite values. No bound on the sum of `tile_mask` on one device may be relied on, other than what follows from the above.
Results may differ from the reference program's by a relative error of at most 0.0028.
Values sent between devices are 32-bit elements; how exact they have to be, the bound alone decides.
A program may use at most 128 MiB of HBM per device.

```python
import math
import jax
import jax.numpy as jnp
from jax import lax

GENES = 32768
COMPONENTS = 128
SKETCH = 128
GENE_TILE = 256
CELL_TILE = 128
SWEEPS = 3
CELLS = 16384
N_GENE = 16


def touch_ends(entries, rng, low, high):
    dims = entries.shape
    index_at = [jax.random.randint(jax.random.fold_in(rng, axis), (), 0, dims[axis]) for axis in range(len(dims))]
    entries = entries.at[tuple(index_at)].set(low)
    longest = dims.index(max(dims))
    index_at[longest] = (index_at[longest] + 1) % dims[longest]
    return entries.at[tuple(index_at)].set(high)


def levels(rng, extent, shards, low, top_value):
    loudness = 1.0
    for position, parts in shards:
        heights = jax.random.uniform(jax.random.fold_in(jax.random.fold_in(rng, 6), position), (parts,), jnp.float32, low / len(shards), top_value / len(shards))
        loudness = loudness * jnp.repeat(jnp.exp(heights), extent[position] // parts).reshape((-1,) + (1,) * (len(extent) - 1 - position))
    return loudness


def gaussian(rng, dims, deviation, limit, shards=(), kind=jnp.bfloat16):
    factor_of = levels(rng, dims, shards, -0.22, 0.18) if shards else 1.0
    drawn = jax.random.normal(rng, dims, jnp.float32) * deviation * factor_of
    return jnp.minimum(jnp.maximum(drawn, -limit), limit).astype(kind)


def setup_inputs(seed: int = 0) -> dict:
    key_of = jax.random.split(jax.random.key(seed), 6)
    counts = gaussian(key_of[0], (GENES, CELLS), 1.0, 6.0, ((0, 16), (1, 8)))
    loadings = gaussian(key_of[1], (GENES, COMPONENTS), GENES ** -0.5, 0.03125, ((0, 16),), jnp.float32)
    values = jnp.clip(jnp.exp(jax.random.uniform(key_of[2], (COMPONENTS,), jnp.float32, math.log(0.5), math.log(2.0))), 0.5, 2.0)
    test_matrix = gaussian(key_of[3], (CELLS, SKETCH), CELLS ** -0.5, 0.046875, ((0, 8),))
    tile_mask = touch_ends((jax.random.randint(key_of[4], (GENES // GENE_TILE, CELLS // CELL_TILE), 0, 4) < 3).astype(jnp.int32), jax.random.fold_in(key_of[4], 1), 0, 1)
    return {"counts": counts, "loadings": loadings, "values": values, "test_matrix": test_matrix, "tile_mask": tile_mask}


def masked_block(count_block, tile_block):
    tile_wide = jnp.repeat(jnp.repeat(tile_block.astype(jnp.bfloat16), GENE_TILE, axis=0), CELL_TILE, axis=1)
    return count_block * tile_wide

def reference(counts, loadings, values, test_matrix, tile_mask):
    highest = lax.Precision.HIGHEST
    gene_rows = GENES // N_GENE
    count_blocks = counts.reshape(N_GENE, gene_rows, CELLS)
    load_blocks = loadings.reshape(N_GENE, gene_rows, COMPONENTS)
    tile_blocks = tile_mask.reshape(N_GENE, gene_rows // GENE_TILE, CELLS // CELL_TILE)

    def project_step(running, inputs):
        count_block, load_block, tile_block = inputs
        masked = masked_block(count_block, tile_block)
        return (running + jnp.dot(load_block.astype(jnp.bfloat16).T.astype(jnp.float32), masked.astype(jnp.float32), preferred_element_type=jnp.float32), None)
    projection, unused = lax.scan(project_step, jnp.zeros((COMPONENTS, CELLS), jnp.float32), (count_blocks, load_blocks, tile_blocks))
    test_wide = test_matrix.astype(jnp.float32)

    def residual_of(count_block, load_block, tile_block):
        masked = masked_block(count_block, tile_block)
        return masked.astype(jnp.float32) - jnp.dot(load_block, projection, precision=highest)

    def sketch_step(inputs):
        count_block, load_block, tile_block = inputs
        return jnp.dot(residual_of(count_block, load_block, tile_block), test_wide, precision=highest)
    sketch = lax.map(sketch_step, (count_blocks, load_blocks, tile_blocks)).reshape(GENES, SKETCH)
    sketch_gram = jnp.dot(sketch.T, sketch, precision=highest)
    factor = jnp.linalg.cholesky(sketch_gram)
    basis = jax.scipy.linalg.solve_triangular(factor, sketch.T, lower=True).T
    basis_blocks = basis.reshape(N_GENE, gene_rows, SKETCH)

    def coef_step(running, inputs):
        count_block, load_block, tile_block, basis_block = inputs
        residual = residual_of(count_block, load_block, tile_block)
        return (running + jnp.dot(basis_block.T, residual, precision=highest), None)
    coef, unused = lax.scan(coef_step, jnp.zeros((SKETCH, CELLS), jnp.float32), (count_blocks, load_blocks, tile_blocks, basis_blocks))
    stacked = jnp.concatenate([projection, coef], axis=0)
    squares = jnp.concatenate([values * values, jnp.zeros((SKETCH,), jnp.float32)])
    core_matrix = jnp.dot(stacked, stacked.T, precision=highest) / CELLS + jnp.diag(squares)
    subspace = jnp.eye(COMPONENTS + SKETCH, COMPONENTS, dtype=jnp.float32)
    for sweep in range(SWEEPS):
        image_block = jnp.dot(core_matrix, subspace, precision=highest)
        chol = jnp.linalg.cholesky(jnp.dot(image_block.T, image_block, precision=highest))
        subspace = jax.scipy.linalg.solve_triangular(chol, image_block.T, lower=True).T
    final_image = jnp.dot(core_matrix, subspace, precision=highest)
    new_values = jnp.sqrt(lax.optimization_barrier(jnp.sum(subspace * final_image, axis=0)))
    rotated = jnp.dot(loadings, subspace[:COMPONENTS], precision=highest) + jnp.dot(basis, subspace[COMPONENTS:], precision=highest)
    new_loadings = rotated * GENES ** 0.5
    return (new_loadings, new_values)
```

```python
import functools
import jax
import jax.numpy as jnp
from jax import lax
from jax.experimental import pallas as pl
from jax.experimental.pallas import tpu as pltpu
from jax.sharding import Mesh
from jax.sharding import PartitionSpec as P

GENE_TILE = 256
CELL_TILE = 128
SWEEPS = 3
BLOCK = 32
CELL = ("cell_0", "cell_1")
GENE = ("gene_0", "gene_1")


def in_blocks(array, dim, length):
    before, after = (array.shape[:dim], array.shape[dim + 1 :])
    return jnp.moveaxis(array.reshape(*before, length, -1, *after), dim, 0)


def sent_and_summed(array, axis, dim):
    length = lax.axis_size(axis)
    parts = lax.all_to_all(in_blocks(array, dim, length), axis, 0, 0, tiled=True)
    return jnp.sum(parts, axis=0)


def padded_to(lines, length):
    spare = -lines.shape[0] % length
    if not spare:
        return lines
    return jnp.concatenate([lines, jnp.zeros((spare, *lines.shape[1:]), lines.dtype)])


def copy_for_each(array, axis):
    copies = jnp.broadcast_to(array, (lax.axis_size(axis), *array.shape))
    return lax.all_to_all(copies, axis, split_axis=0, concat_axis=0, tiled=True)


def joined_along(parts, dim):
    parts = jnp.moveaxis(parts, 0, dim)
    shape = parts.shape
    return parts.reshape(*shape[:dim], shape[dim] * shape[dim + 1], *shape[dim + 2 :])


def gather_directly(array, axis, dim):
    parts = copy_for_each(array, axis)
    return joined_along(parts, dim)


def sum_by_parts(array, axes):
    lines = array.reshape(-1, array.shape[-1])
    own = sent_and_summed(padded_to(lines, lax.axis_size(axes)), axes, 0)
    whole = gather_directly(own, axes, 0)
    return whole[: len(lines)].reshape(array.shape)


def total_of_pieces(array, axis):
    return lax.all_gather(array, axis).sum(0)


def sum_by_axis(array, axes, dim):
    far, near = axes
    own = sent_and_summed(in_blocks(array, dim, lax.axis_size(far)), near, dim + 1)
    return jnp.sum(lax.all_to_all(own, far, 0, 0, tiled=True), axis=0)


def gather_axes(array, axes, dim):
    far, near = axes
    leading = copy_for_each(array, far)
    parts = jnp.swapaxes(copy_for_each(leading, near), 0, 1)
    return joined_along(parts.reshape(-1, *array.shape), dim)


def nested_sum(array, axes):
    own = sum_by_axis(padded_to(array, lax.axis_size(axes[0]) * lax.axis_size(axes[1])), axes, 0)
    whole = gather_axes(own, axes, 0)
    return whole[: len(array)].reshape(array.shape)


def in_one(arrays, axis):
    vector, at, finished = (jnp.concatenate([a.reshape(-1) for a in arrays]), 0, [])
    total = nested_sum(vector, axis)
    for a in arrays:
        finished.append(total[at : at + a.size].reshape(a.shape))
        at += a.size
    return tuple(finished)


def contract(left, right):
    return lax.dot_general(
        left,
        right,
        (((0,), (0,)), ((), ())),
        precision=lax.Precision.HIGHEST,
        preferred_element_type=jnp.float32,
    )


def outer_rows(stacked):
    return lax.dot_general(
        stacked,
        stacked,
        (((1,), (1,)), ((), ())),
        precision=lax.Precision.HIGHEST,
        preferred_element_type=jnp.float32,
    )


def dot(left, right, left_dim, right_dim):
    return lax.dot_general(
        left,
        right,
        (((left_dim,), (right_dim,)), ((), ())),
        precision=lax.Precision.HIGHEST,
        preferred_element_type=jnp.float32,
    )


def identity(size):
    row = lax.broadcasted_iota(jnp.int32, (size, size), 0)
    column = lax.broadcasted_iota(jnp.int32, (size, size), 1)
    return jnp.where(row == column, 1.0, 0.0).astype(jnp.float32)


def inverse_factor(work, gram):
    size = gram.shape[0]
    work[:, :size] = gram
    work[:, size:] = identity(size)
    row_of = lax.broadcasted_iota(jnp.int32, (BLOCK, size), 0)
    for start in range(0, size, BLOCK):
        panel = work[start : start + BLOCK, :]
        columns = [
            jnp.broadcast_to(panel[:, start + j : start + j + 1], (BLOCK, size))
            for j in range(BLOCK)
        ]
        halves = [panel[:, :size], panel[:, size:]]
        pivots = jnp.zeros((BLOCK, size), jnp.float32)
        for j in range(BLOCK):
            column = columns[j]
            spread = jnp.broadcast_to(column[j : j + 1], (BLOCK, size))
            inverse = 1.0 / spread
            pivots = jnp.where(row_of == j, spread, pivots)
            for k in range(j + 1, BLOCK):
                lead = jnp.broadcast_to(column[k : k + 1], (BLOCK, size))
                columns[k] = columns[k] - column * (lead * inverse)
            ratio = jnp.where(row_of > j, column * inverse, 0.0)
            halves = [h - ratio * jnp.broadcast_to(h[j : j + 1], (BLOCK, size)) for h in halves]
        scale = lax.rsqrt(pivots)
        panel = jnp.concatenate([h * scale for h in halves], axis=1)
        work[start : start + BLOCK, :] = panel
        if start + BLOCK < size:
            update = dot(panel[:, :size], panel, 0, 0)
            work[start + BLOCK :, :] = work[start + BLOCK :, :] - update[start + BLOCK :, :]
    return work[:, size:]


def subspace_kernel(
    cells_total, core_ref, gram_ref, values_ref, top_ref, bottom_ref, squares_ref, work, core, subspace, basis
):
    size = gram_ref.shape[0]
    basis[...] = inverse_factor(work, gram_ref[...])
    inverse = basis[...]
    values = values_ref[...]
    cross = dot(inverse, core_ref[size:, :size], 1, 0)
    corner = dot(dot(inverse, core_ref[size:, size:], 1, 0), inverse, 1, 1)
    squares = jnp.broadcast_to(values * values, (size, size)) * identity(size)
    core[:size, :size] = core_ref[:size, :size] / cells_total + squares
    core[size:, :size] = cross / cells_total
    core[:size, size:] = dot(core_ref[:size, size:], inverse, 1, 1) / cells_total
    core[size:, size:] = corner / cells_total
    subspace[:size] = identity(size)
    subspace[size:] = jnp.zeros((size, size), jnp.float32)

    def sweep(step, carry):
        image = dot(core[...], subspace[...], 1, 0)
        rotation = inverse_factor(work, dot(image, image, 0, 0))
        subspace[...] = dot(image, rotation, 1, 1)
        return carry

    lax.fori_loop(0, SWEEPS, sweep, 0)
    final = dot(core[...], subspace[...], 1, 0)
    squares_ref[...] = jnp.sum(subspace[...] * final, axis=0, keepdims=True)
    top_ref[...] = subspace[:size]
    bottom_ref[...] = dot(basis[...], subspace[size:], 0, 0)


def subspace_call(core_raw, gram, values, cells_total):
    size = gram.shape[0]
    shape = lambda *dims: jax.ShapeDtypeStruct(dims, jnp.float32)
    return pl.pallas_call(
        functools.partial(subspace_kernel, cells_total),
        out_shape=(shape(size, size), shape(size, size), shape(1, size)),
        scratch_shapes=[
            pltpu.VMEM((size, 2 * size), jnp.float32),
            pltpu.VMEM((2 * size, 2 * size), jnp.float32),
            pltpu.VMEM((2 * size, size), jnp.float32),
            pltpu.VMEM((size, size), jnp.float32),
        ],
        name="subspace",
    )(core_raw, gram, values.reshape(1, size))


def local(counts, loadings, values, test_matrix, tile_mask):
    highest = lax.Precision.HIGHEST
    gene_rows, cell_cols = counts.shape
    components = loadings.shape[1]
    sketch_width = test_matrix.shape[1]
    cells_total = cell_cols * lax.axis_size(CELL)
    genes_total = gene_rows * lax.axis_size(GENE)
    tile_wide = jnp.repeat(
        jnp.repeat(tile_mask.astype(jnp.bfloat16), GENE_TILE, axis=0), CELL_TILE, axis=1
    )
    masked = counts * tile_wide
    load_narrow = loadings.astype(jnp.bfloat16)
    proj_part = lax.dot_general(
        load_narrow, masked, (((0,), (0,)), ((), ())), preferred_element_type=jnp.float32
    )
    projection = sum_by_parts(proj_part, GENE)
    test_wide = test_matrix.astype(jnp.float32)
    raw_part = jnp.dot(masked, test_matrix, preferred_element_type=jnp.float32)
    small_part = jnp.dot(projection, test_wide, precision=highest)
    raw_sketch, small_sketch = (total_of_pieces(raw_part, CELL), total_of_pieces(small_part, CELL))
    sketch = raw_sketch - jnp.dot(loadings, small_sketch, precision=highest)
    rows_left = sketch.T
    along_loadings = jnp.dot(rows_left, loadings, precision=highest)
    inner = sent_and_summed(
        jnp.dot(rows_left, masked, precision=highest, preferred_element_type=jnp.float32)
        - jnp.dot(along_loadings, projection, precision=highest),
        GENE,
        1,
    )
    share_width = inner.shape[1]
    offset = lax.axis_index(GENE) * share_width
    proj_share = lax.dynamic_slice_in_dim(projection, offset, share_width, 1)
    test_share = lax.dynamic_slice_in_dim(test_wide, offset, share_width, 0)
    stacked = jnp.concatenate([proj_share, inner], axis=0)
    gram_part = jnp.dot(inner, test_share, precision=highest)
    core_raw, sketch_gram = in_one(
        (outer_rows(stacked), gram_part), (("gene_0", "gene_1", "cell_0"), "cell_1")
    )
    top, bottom, squares_out = subspace_call(core_raw, sketch_gram, values, cells_total)
    rotated = jnp.dot(loadings, top, precision=highest) + jnp.dot(
        sketch, bottom, precision=highest
    )
    new_loadings = rotated * genes_total**0.5
    return (new_loadings, jnp.sqrt(squares_out[0]))


def solution(mesh):
    torus = Mesh(mesh.devices.reshape(4, 4, 4, 2), ("gene_0", "gene_1", "cell_0", "cell_1"))
    placed = (P(GENE, CELL), P(GENE, None), P(), P(CELL, None), P(GENE, CELL))
    return jax.shard_map(
        local, mesh=torus, in_specs=placed, out_specs=(P(GENE, None), P()), check_vma=False
    )
```

```python
import functools
import jax
import jax.numpy as jnp
from jax import lax
from jax.experimental import pallas as pl
from jax.experimental.pallas import tpu as pltpu
from jax.sharding import Mesh
from jax.sharding import PartitionSpec as P

GENE_TILE = 256
CELL_TILE = 128
SWEEPS = 3
BLOCK = 32
CELL = ("cell_0", "cell_1")
GENE = ("gene_0", "gene_1")


AXES = (*GENE, *CELL)


def dot(left, right, left_dim, right_dim):
    return lax.dot_general(
        left,
        right,
        (((left_dim,), (right_dim,)), ((), ())),
        precision=lax.Precision.HIGHEST,
        preferred_element_type=jnp.float32,
    )


def identity(size):
    row = lax.broadcasted_iota(jnp.int32, (size, size), 0)
    column = lax.broadcasted_iota(jnp.int32, (size, size), 1)
    return jnp.where(row == column, 1.0, 0.0).astype(jnp.float32)


def inverse_factor(work, gram):
    size = gram.shape[0]
    work[:, :size] = gram
    work[:, size:] = identity(size)
    row_of = lax.broadcasted_iota(jnp.int32, (BLOCK, size), 0)
    for start in range(0, size, BLOCK):
        panel = work[start : start + BLOCK, :]
        columns = [
            jnp.broadcast_to(panel[:, start + j : start + j + 1], (BLOCK, size))
            for j in range(BLOCK)
        ]
        halves = [panel[:, :size], panel[:, size:]]
        pivots = jnp.zeros((BLOCK, size), jnp.float32)
        for j in range(BLOCK):
            column = columns[j]
            spread = jnp.broadcast_to(column[j : j + 1], (BLOCK, size))
            inverse = 1.0 / spread
            pivots = jnp.where(row_of == j, spread, pivots)
            for k in range(j + 1, BLOCK):
                lead = jnp.broadcast_to(column[k : k + 1], (BLOCK, size))
                columns[k] = columns[k] - column * (lead * inverse)
            ratio = jnp.where(row_of > j, column * inverse, 0.0)
            halves = [h - ratio * jnp.broadcast_to(h[j : j + 1], (BLOCK, size)) for h in halves]
        scale = lax.rsqrt(pivots)
        panel = jnp.concatenate([h * scale for h in halves], axis=1)
        work[start : start + BLOCK, :] = panel
        if start + BLOCK < size:
            update = dot(panel[:, :size], panel, 0, 0)
            work[start + BLOCK :, :] = work[start + BLOCK :, :] - update[start + BLOCK :, :]
    return work[:, size:]


def group_kernel(
    genes_local,
    counts_ref, loadings_ref, test_ref, tile_ref,
    sketch_ref, core_ref, gram_ref,
    masked, narrow, wide, split, turned, y_part, y_pair, y_ring, y_full,
    q_part, q_cell, q_gene, q_full, p_send, p_recv, z_send, z_recv,
    t_recv, t_full, c_send, c_recv, c_cell, c_full,
    load_sem, pair_sem, ring_sem, full_sem, send_sem, recv_sem,
):
    z, x, y, k = (lax.axis_index(a) for a in AXES)
    gene, cell = z * 4 + x, y * 2 + k
    f32, bf16 = jnp.float32, jnp.bfloat16
    rows = genes_local // 8
    gene_steps = [(a, b) for a in range(4) for b in range(4)][1:]
    cell_steps = [(a, b) for a in range(4) for b in range(2)][1:]

    def gene_at(step):
        return lax.rem(z + step[0], 4), lax.rem(x + step[1], 4)

    def cell_at(step):
        return lax.rem(y + step[0], 4), lax.rem(k + step[1], 2)

    def gene_device(at):
        return {"gene_0": at[0], "gene_1": at[1]}

    def cell_device(at):
        return {"cell_0": at[0], "cell_1": at[1]}

    def copy(source, target, sent, arrived, device):
        return pltpu.make_async_remote_copy(
            src_ref=source, dst_ref=target, send_sem=sent, recv_sem=arrived,
            device_id=device, device_id_type=pl.DeviceIdType.MESH,
        )

    partner = {"cell_1": 1 - k}

    def sent(ref, sem):
        copy(ref, ref, sem, sem, partner).wait_send()

    def arrived(ref, sem):
        copy(ref, ref, sem, sem, partner).wait_recv()

    def to_genes(phase, piece, target):
        for step in gene_steps:
            at = gene_at(step)
            copy(piece(at[0] * 4 + at[1]), target, send_sem.at[phase], recv_sem.at[phase],
                 gene_device(at)).start()

    def to_cells(phase, piece, target):
        for step in cell_steps:
            at = cell_at(step)
            copy(piece(at[0] * 2 + at[1]), target, send_sem.at[phase], recv_sem.at[phase],
                 cell_device(at)).start()

    loads = [
        pltpu.make_async_copy(
            counts_ref.at[pl.ds(t * rows, rows)], masked.at[pl.ds(t * rows, rows)], load_sem.at[t]
        )
        for t in range(8)
    ]
    for load in loads:
        load.start()
    barrier = pltpu.get_barrier_semaphore()
    for step in gene_steps:
        pl.semaphore_signal(barrier, inc=1, device_id=gene_device(gene_at(step)),
                            device_id_type=pl.DeviceIdType.MESH)
    for step in cell_steps:
        pl.semaphore_signal(barrier, inc=1, device_id=cell_device(cell_at(step)),
                            device_id_type=pl.DeviceIdType.MESH)
    narrow[...] = loadings_ref[...].T.astype(bf16)
    pl.semaphore_wait(barrier, len(gene_steps) + len(cell_steps))

    for t in range(8):
        loads[t].wait()
        for c in range(tile_ref.shape[1]):
            at = (slice(t * rows, (t + 1) * rows), slice(c * CELL_TILE, (c + 1) * CELL_TILE))
            block = masked[at]
            masked[at] = jnp.where(tile_ref[t, c] != 0, block, jnp.zeros_like(block))
        y_part[t] = jnp.dot(masked[t * rows:(t + 1) * rows], test_ref[...], preferred_element_type=f32)
        if t % 2:
            copy(y_part.at[t - k], y_pair.at[t // 2], pair_sem.at[0, t // 2], pair_sem.at[1, t // 2],
                 partner).start()

    high = y_part[...].reshape(genes_local, 128)
    wide[:, :128] = high.astype(bf16)
    wide[:, 128:] = (high - wide[:, :128].astype(f32)).astype(bf16)
    both = jnp.dot(narrow[...], wide[...], preferred_element_type=f32)
    q_part[...] = (both[:, :128] + both[:, 128:]).reshape(8, 16, 128)
    to_cells(0, lambda at: q_part.at[at], q_cell.at[cell])
    q_cell[cell] = q_part[cell]

    for t in range(4):
        arrived(y_pair.at[t], pair_sem.at[1, t])
        y_pair[t] = y_pair[t] + y_part[2 * t + k]
    for step in (1, 3, 2):
        to = lax.rem(y + step, 4)
        copy(y_pair.at[to], y_ring.at[y], ring_sem.at[0, step], ring_sem.at[1, y], {"cell_0": to}).start()
    y_ring[y] = y_pair[y]

    def project(e, carry):
        pair = lax.rem(gene // 2 + e, 8)
        lanes = pl.ds(pl.multiple_of(pair * 256, 256), 256)
        part = jnp.dot(narrow[...], masked[:, lanes], preferred_element_type=f32)
        p_send[2 * pair] = part[:, :128]
        p_send[2 * pair + 1] = part[:, 128:]
        return carry

    lax.fori_loop(0, 8, project, 0)
    arrived(q_cell.at[pl.ds(0, 7)], recv_sem.at[0])
    q_gene[gene] = jnp.sum(q_cell[...], axis=0)
    to_genes(1, lambda at: q_gene.at[gene], q_gene.at[gene])
    to_genes(2, lambda at: p_send.at[at], p_recv.at[gene])
    p_recv[gene] = p_send[gene]

    for step in (1, 2, 3):
        source = lax.rem(y + step, 4)
        arrived(y_ring.at[source], ring_sem.at[1, source])
    y_full[cell] = jnp.sum(y_ring[...], axis=0)
    for step in (1, 3, 2):
        to = lax.rem(y + step, 4)
        copy(y_full.at[cell], y_full.at[cell], full_sem.at[0, step], full_sem.at[1, cell], {"cell_0": to}).start()
    copy(y_full.at[cell], y_full.at[cell], full_sem.at[0, 0], full_sem.at[1, cell], partner).start()

    arrived(q_gene.at[pl.ds(0, 15)], recv_sem.at[1])
    q_full[cell] = jnp.sum(q_gene[...], axis=0)
    to_cells(3, lambda at: q_full.at[cell], q_full.at[cell])
    arrived(q_full.at[pl.ds(0, 7)], recv_sem.at[3])
    sketch_ref[...] = dot(loadings_ref[...], q_full[...].reshape(128, 128), 1, 0)
    for step in (1, 3, 2):
        source = lax.rem(y + step, 4) * 2 + k
        arrived(y_full.at[source], full_sem.at[1, source])
        copy(y_full.at[source], y_full.at[source], full_sem.at[0, 3 + step], full_sem.at[1, source],
             partner).start()
    for step in (0, 1, 3, 2):
        source = lax.rem(y + step, 4) * 2 + 1 - k
        arrived(y_full.at[source], full_sem.at[1, source])

    sketch_ref[...] = y_full[...].reshape(genes_local, 128) - sketch_ref[...]
    turned[...] = sketch_ref[...].T
    split[:128] = turned[...].astype(bf16)
    split[128:] = (turned[...] - split[:128].astype(f32)).astype(bf16)
    own = turned[pl.ds(pl.multiple_of(16 * cell, 16), 16), :]
    t_recv[gene, :, :128] = dot(own, loadings_ref[...], 1, 0)
    t_recv[gene, :, 128:] = dot(own, sketch_ref[...], 1, 0)
    to_genes(4, lambda at: t_recv.at[gene], t_recv.at[gene])

    def inner(e, carry):
        pair = lax.rem(gene // 2 + e, 8)
        lanes = pl.ds(pl.multiple_of(pair * 256, 256), 256)
        part = jnp.dot(split[...], masked[:, lanes], preferred_element_type=f32)
        part = part[:128] + part[128:]
        z_send[2 * pair] = part[:, :128]
        z_send[2 * pair + 1] = part[:, 128:]
        return carry

    def send_inner(at):
        copy(z_send.at[at], z_recv.at[gene], send_sem.at[5], recv_sem.at[5],
             {"gene_0": at // 4, "gene_1": lax.rem(at, 4)}).start()

    def inner_and_send(e, carry):
        inner(e, carry)
        pair = lax.rem(gene // 2 + e, 8)
        send_inner(2 * pair)
        send_inner(2 * pair + 1)
        return carry

    lax.fori_loop(1, 8, inner_and_send, 0)
    inner(0, 0)
    send_inner(gene + 1 - 2 * lax.rem(gene, 2))
    z_recv[gene] = z_send[gene]

    arrived(t_recv.at[pl.ds(0, 15)], recv_sem.at[4])
    t_full[cell] = jnp.sum(t_recv[...], axis=0)
    to_cells(6, lambda at: t_full.at[cell], t_full.at[cell])
    arrived(t_full.at[pl.ds(0, 7)], recv_sem.at[6])
    whole = t_full[...].reshape(128, 256)
    gram_ref[...] = whole[:, 128:]

    arrived(p_recv.at[pl.ds(0, 15)], recv_sem.at[2])
    projection = jnp.sum(p_recv[...], axis=0)
    arrived(z_recv.at[pl.ds(0, 15)], recv_sem.at[5])
    residual = jnp.sum(z_recv[...], axis=0) - dot(whole[:, :128], projection, 1, 0)
    c_send[:, :8] = dot(projection, projection, 1, 1).reshape(16, 8, 128)
    c_send[:, 8:16] = dot(residual, projection, 1, 1).reshape(16, 8, 128)
    c_send[:, 16:] = dot(residual, residual, 1, 1).reshape(16, 8, 128)
    to_genes(7, lambda at: c_send.at[at], c_recv.at[gene])
    c_recv[gene] = c_send[gene]
    arrived(c_recv.at[pl.ds(0, 15)], recv_sem.at[7])
    c_cell[cell] = jnp.sum(c_recv[...], axis=0)
    to_cells(8, lambda at: c_cell.at[cell], c_cell.at[cell])
    arrived(c_cell.at[pl.ds(0, 7)], recv_sem.at[8])
    c_full[gene] = jnp.sum(c_cell[...], axis=0)
    to_genes(9, lambda at: c_full.at[gene], c_full.at[gene])
    arrived(c_full.at[pl.ds(0, 15)], recv_sem.at[9])
    for part in range(3):
        core_ref[part] = c_full[:, 8 * part:8 * part + 8].reshape(128, 128)

    for t in range(4):
        sent(y_pair.at[t], pair_sem.at[0, t])
    for step in (1, 2, 3):
        sent(y_pair.at[0], ring_sem.at[0, step])
    for step in range(7):
        sent(y_full.at[0], full_sem.at[0, step])
    sent(q_cell.at[pl.ds(0, 7)], send_sem.at[0])
    sent(q_gene.at[pl.ds(0, 15)], send_sem.at[1])
    sent(p_recv.at[pl.ds(0, 15)], send_sem.at[2])
    sent(q_full.at[pl.ds(0, 7)], send_sem.at[3])
    sent(t_recv.at[pl.ds(0, 15)], send_sem.at[4])
    sent(z_recv.at[pl.ds(0, 15)], send_sem.at[5])
    sent(t_full.at[pl.ds(0, 7)], send_sem.at[6])
    sent(c_recv.at[pl.ds(0, 15)], send_sem.at[7])
    sent(c_cell.at[pl.ds(0, 7)], send_sem.at[8])
    sent(c_full.at[pl.ds(0, 15)], send_sem.at[9])


def group_call(counts, loadings, test_matrix, tile_mask):
    f32, bf16 = jnp.float32, jnp.bfloat16
    genes, cells = counts.shape
    whole = pl.BlockSpec(memory_space=pltpu.VMEM)
    dma = pltpu.SemaphoreType.DMA
    return pl.pallas_call(
        functools.partial(group_kernel, genes),
        out_shape=(
            jax.ShapeDtypeStruct((genes, 128), f32),
            jax.ShapeDtypeStruct((3, 128, 128), f32),
            jax.ShapeDtypeStruct((128, 128), f32),
        ),
        in_specs=[
            pl.BlockSpec(memory_space=pltpu.HBM),
            whole,
            whole,
            pl.BlockSpec(memory_space=pltpu.SMEM),
        ],
        out_specs=(whole, whole, whole),
        scratch_shapes=[
            pltpu.VMEM((genes, cells), bf16),
            pltpu.VMEM((128, genes), bf16),
            pltpu.VMEM((genes, 256), bf16),
            pltpu.VMEM((256, genes), bf16),
            pltpu.VMEM((128, genes), f32),
            pltpu.VMEM((8, genes // 8, 128), f32),
            pltpu.VMEM((4, genes // 8, 128), f32),
            pltpu.VMEM((4, genes // 8, 128), f32),
            pltpu.VMEM((8, genes // 8, 128), f32),
            pltpu.VMEM((8, 16, 128), f32),
            pltpu.VMEM((8, 16, 128), f32),
            pltpu.VMEM((16, 16, 128), f32),
            pltpu.VMEM((8, 16, 128), f32),
            pltpu.VMEM((16, 128, cells // 16), f32),
            pltpu.VMEM((16, 128, cells // 16), f32),
            pltpu.VMEM((16, 128, cells // 16), f32),
            pltpu.VMEM((16, 128, cells // 16), f32),
            pltpu.VMEM((16, 16, 256), f32),
            pltpu.VMEM((8, 16, 256), f32),
            pltpu.VMEM((16, 24, 128), f32),
            pltpu.VMEM((16, 24, 128), f32),
            pltpu.VMEM((8, 24, 128), f32),
            pltpu.VMEM((16, 24, 128), f32),
            dma((8,)),
            dma((2, 4)),
            dma((2, 4)),
            dma((2, 8)),
            dma((10,)),
            dma((10,)),
        ],
        compiler_params=pltpu.CompilerParams(
            collective_id=0, has_side_effects=True, vmem_limit_bytes=60 * 1024 * 1024
        ),
        name="group",
    )(counts, loadings, test_matrix, tile_mask)


def subspace_kernel(
    cells_total, genes_total, core_ref, gram_ref, values_ref, loadings_ref, sketch_ref,
    out_ref, squares_ref, work, core, subspace, basis,
):
    size = gram_ref.shape[0]
    basis[...] = inverse_factor(work, gram_ref[...])
    inverse = basis[...]
    values = values_ref[...]
    cross = dot(inverse, core_ref[1], 1, 0) / cells_total
    corner = dot(dot(inverse, core_ref[2], 1, 0), inverse, 1, 1)
    squares = jnp.broadcast_to(values * values, (size, size)) * identity(size)
    core[:size, :size] = core_ref[0] / cells_total + squares
    core[size:, :size] = cross
    core[:size, size:] = cross.T
    core[size:, size:] = corner / cells_total
    subspace[:size] = identity(size)
    subspace[size:] = jnp.zeros((size, size), jnp.float32)

    def sweep(step, carry):
        image = dot(core[...], subspace[...], 1, 0)
        rotation = inverse_factor(work, dot(image, image, 0, 0))
        subspace[...] = dot(image, rotation, 1, 1)
        return carry

    lax.fori_loop(0, SWEEPS, sweep, 0)
    final = dot(core[...], subspace[...], 1, 0)
    squares_ref[...] = jnp.sum(subspace[...] * final, axis=0, keepdims=True)
    top = subspace[:size]
    bottom = dot(basis[...], subspace[size:], 0, 0)
    rotated = dot(loadings_ref[...], top, 1, 0) + dot(sketch_ref[...], bottom, 1, 0)
    out_ref[...] = rotated * genes_total**0.5


def subspace_call(core, gram, values, loadings, sketch, cells_total, genes_total):
    size = gram.shape[0]
    return pl.pallas_call(
        functools.partial(subspace_kernel, cells_total, genes_total),
        out_shape=(
            jax.ShapeDtypeStruct(loadings.shape, jnp.float32),
            jax.ShapeDtypeStruct((1, size), jnp.float32),
        ),
        scratch_shapes=[
            pltpu.VMEM((size, 2 * size), jnp.float32),
            pltpu.VMEM((2 * size, 2 * size), jnp.float32),
            pltpu.VMEM((2 * size, size), jnp.float32),
            pltpu.VMEM((size, size), jnp.float32),
        ],
        name="subspace",
    )(core, gram, values.reshape(1, size), loadings, sketch)


def local(counts, loadings, values, test_matrix, tile_mask):
    cells_total = counts.shape[1] * lax.axis_size(CELL)
    genes_total = counts.shape[0] * lax.axis_size(GENE)
    sketch, core, gram = group_call(counts, loadings, test_matrix, tile_mask)
    new_loadings, squares = subspace_call(
        core, gram, values, loadings, sketch, cells_total, genes_total
    )
    return (new_loadings, jnp.sqrt(squares[0]))


def solution(mesh):
    torus = Mesh(mesh.devices.reshape(4, 4, 4, 2), ("gene_0", "gene_1", "cell_0", "cell_1"))
    placed = (P(GENE, CELL), P(GENE, None), P(), P(CELL, None), P(GENE, CELL))
    return jax.shard_map(
        local, mesh=torus, in_specs=placed, out_specs=(P(GENE, None), P()), check_vma=False
    )
```

```python
import functools
import jax
import jax.numpy as jnp
from jax import lax
from jax.experimental import pallas as pl
from jax.experimental.pallas import tpu as pltpu
from jax.sharding import Mesh
from jax.sharding import PartitionSpec as P

GENE_TILE = 256
CELL_TILE = 128
SWEEPS = 3
BLOCK = 32
COLUMNS = 16
GROUP_VMEM = 52 * 1024 * 1024
CELL = ("cell_0", "cell_1")
GENE = ("gene_0", "gene_1")


AXES = (*GENE, *CELL)


def dot(left, right, left_dim, right_dim):
    return lax.dot_general(
        left,
        right,
        (((left_dim,), (right_dim,)), ((), ())),
        precision=lax.Precision.HIGHEST,
        preferred_element_type=jnp.float32,
    )


def identity(size):
    row = lax.broadcasted_iota(jnp.int32, (size, size), 0)
    column = lax.broadcasted_iota(jnp.int32, (size, size), 1)
    return jnp.where(row == column, 1.0, 0.0).astype(jnp.float32)


def three_parts(array):
    first = array.astype(jnp.bfloat16)
    rest = array - first.astype(jnp.float32)
    second = rest.astype(jnp.bfloat16)
    return first, second, (rest - second.astype(jnp.float32)).astype(jnp.bfloat16)


def left_parts(array, dim):
    a, b, c = three_parts(array)
    return jnp.concatenate([a, a, b, a, b, c], axis=dim)


def right_parts(array, dim):
    a, b, c = three_parts(array)
    return jnp.concatenate([a, b, a, c, b, a], axis=dim)


def of_parts(left, right, left_dim=1):
    return lax.dot_general(
        left, right, (((left_dim,), (0,)), ((), ())), preferred_element_type=jnp.float32
    )


def inverse_factor(work, gram):
    size = gram.shape[0]
    groups = range(BLOCK // 8)
    work[:, :size] = gram
    work[:, size:] = identity(size)
    row_of = lax.broadcasted_iota(jnp.int32, (8, size), 0)

    def spread(rows, at):
        return jnp.broadcast_to(rows[at : at + 1], (8, size))

    for start in range(0, size, BLOCK):
        halves = [
            [work[start + 8 * g : start + 8 * g + 8, h : h + size] for g in groups]
            for h in (0, size)
        ]
        pivots = [jnp.zeros((8, size), jnp.float32) for g in groups]
        for j in range(BLOCK):
            own, at = j // 8, j % 8
            if j % COLUMNS == 0:
                columns = {
                    k: {
                        g: jnp.broadcast_to(halves[0][g][:, start + k : start + k + 1], (8, size))
                        for g in groups[k // 8 :]
                    }
                    for k in range(j, j + COLUMNS)
                }
                pivot = spread(columns[j][own], at)
                inverse = 1.0 / pivot
            pivots[own] = jnp.where(row_of == at, pivot, pivots[own])
            ratios = {g: c * inverse for g, c in columns[j].items()}
            others = range(j + 1, j - j % COLUMNS + COLUMNS)
            if others:
                after, below = (j + 1) // 8, (j + 1) % 8
                edge = spread(columns[j][after], below)
                first = edge * inverse
                pivot = spread(columns[j + 1][after], below) - edge * first
                inverse = 1.0 / pivot
            for k in others:
                lead = first if k == j + 1 else spread(ratios[k // 8], k % 8)
                for g in groups[k // 8 :]:
                    columns[k][g] = columns[k][g] - columns[j][g] * lead
            ratios[own] = jnp.where(row_of > at, ratios[own], 0.0)
            for half in halves:
                top = spread(half[own], at)
                for g in groups[own:]:
                    half[g] = half[g] - ratios[g] * top
        scales = [lax.rsqrt(pivot) for pivot in pivots]
        panel = jnp.concatenate(
            [jnp.concatenate([half[g] * scales[g] for g in groups], axis=0) for half in halves],
            axis=1,
        )
        work[start : start + BLOCK, :] = panel
        if start + BLOCK < size:
            update = of_parts(left_parts(panel[:, :size], 0), right_parts(panel, 0), 0)
            work[start + BLOCK :, :] = work[start + BLOCK :, :] - update[start + BLOCK :, :]
    return work[:, size:]


def group_kernel(
    genes_local, cells_total, genes_total,
    counts_ref, loadings_hbm, test_ref, tile_ref, values_ref,
    out_ref, singular_ref,
    loadings_ref, high_ref, low_ref, core, basis_ref, image,
    masked, narrow, wide, split, fitted, work, y_part, y_pair, y_ring, y_full,
    q_part, q_cell, q_gene, q_full, p_send, p_one, p_mid, p_two, z_send, z_one, z_mid, z_two,
    t_one, t_two, t_full, c_send, c_recv, c_cell, c_full,
    load_sem, pair_sem, ring_sem, full_sem, send_sem, recv_sem,
):
    z, x, y, k = (lax.axis_index(a) for a in AXES)
    gene, cell = z * 4 + x, y * 2 + k
    near, far = z + k * (x - z), x + k * (z - x)
    f32, bf16 = jnp.float32, jnp.bfloat16
    rows = genes_local // 8
    gene_steps = [(m, n) for m in range(4) for n in range(4)][1:]
    cell_steps = [(m, n) for m in range(4) for n in range(2)][1:]

    def gene_at(step):
        return lax.rem(z + step[0], 4), lax.rem(x + step[1], 4)

    def cell_at(step):
        return lax.rem(y + step[0], 4), lax.rem(k + step[1], 2)

    def gene_device(at):
        return {"gene_0": at[0], "gene_1": at[1]}

    def cell_device(at):
        return {"cell_0": at[0], "cell_1": at[1]}

    def line_device(first, second):
        return gene_device((first + k * (second - first), second + k * (first - second)))

    def copy(source, target, sent, arrived, device):
        return pltpu.make_async_remote_copy(
            src_ref=source, dst_ref=target, send_sem=sent, recv_sem=arrived,
            device_id=device, device_id_type=pl.DeviceIdType.MESH,
        )

    partner = {"cell_1": 1 - k}

    def sent(ref, sem):
        copy(ref, ref, sem, sem, partner).wait_send()

    def arrived(ref, sem):
        copy(ref, ref, sem, sem, partner).wait_recv()

    def to_genes(phase, piece, target):
        for step in gene_steps:
            at = gene_at(step)
            copy(piece(at[0] * 4 + at[1]), target, send_sem.at[phase], recv_sem.at[phase],
                 gene_device(at)).start()

    def to_cells(phase, piece, target):
        for step in cell_steps:
            at = cell_at(step)
            copy(piece(at[0] * 2 + at[1]), target, send_sem.at[phase], recv_sem.at[phase],
                 cell_device(at)).start()

    def to_near(phase, at, source, target):
        copy(source, target, send_sem.at[phase], recv_sem.at[phase], line_device(at, far)).start()

    def to_far(phase, at, source, target):
        copy(source, target, send_sem.at[phase], recv_sem.at[phase], line_device(near, at)).start()

    def three(ref):
        return ref.at[pl.ds(0, 3)]

    order = [lax.rem(y + step, 4) for step in (2, 1, 3, 0)]
    tiles = [2 * at + lax.rem(k + turn, 2) for at in order for turn in (1, 0)]

    def load(t):
        at = pl.ds(pl.multiple_of(t * rows, rows), rows)
        return pltpu.make_async_copy(counts_ref.at[at], masked.at[at], load_sem.at[t])

    loadings_copy = pltpu.make_async_copy(loadings_hbm, loadings_ref, load_sem.at[8])
    for t in tiles[:2]:
        load(t).start()
    loadings_copy.start()
    for t in tiles[2:]:
        load(t).start()
    barrier = pltpu.get_barrier_semaphore()
    for step in gene_steps:
        pl.semaphore_signal(barrier, inc=1, device_id=gene_device(gene_at(step)),
                            device_id_type=pl.DeviceIdType.MESH)
    for step in cell_steps:
        pl.semaphore_signal(barrier, inc=1, device_id=cell_device(cell_at(step)),
                            device_id_type=pl.DeviceIdType.MESH)
    def sketch_rows(t):
        load(t).wait()
        at = pl.ds(pl.multiple_of(t * rows, rows), rows)
        for c in range(tile_ref.shape[1]):
            lanes = slice(c * CELL_TILE, (c + 1) * CELL_TILE)
            block = masked[at, lanes]
            masked[at, lanes] = jnp.where(tile_ref[t, c] != 0, block, jnp.zeros_like(block))
        y_part[t] = jnp.dot(masked[at], test_ref[...], preferred_element_type=f32)

    def pair_sum(n):
        arrived(y_pair.at[order[n]], pair_sem.at[1, order[n]])
        y_pair[order[n]] = y_pair[order[n]] + y_part[2 * order[n] + k]

    def send_along(n):
        pair_sum(n)
        copy(y_pair.at[order[n]], y_ring.at[y], ring_sem.at[0, n], ring_sem.at[1, y],
             {"cell_0": order[n]}).start()

    sketch_rows(tiles[0])
    loadings_copy.wait()
    high_ref[:, :128] = loadings_ref[...].astype(bf16)
    narrow[...] = high_ref[:, :128].T
    pl.semaphore_wait(barrier, len(gene_steps) + len(cell_steps))
    for n in range(4):
        if n:
            sketch_rows(tiles[2 * n])
        copy(y_part.at[tiles[2 * n]], y_pair.at[order[n]], pair_sem.at[0, n],
             pair_sem.at[1, order[n]], partner).start()
        sketch_rows(tiles[2 * n + 1])
        if n:
            send_along(n - 1)

    whole = y_part[...].reshape(genes_local, 128)
    wide[:, :128] = whole.astype(bf16)
    wide[:, 128:] = (whole - wide[:, :128].astype(f32)).astype(bf16)
    both = jnp.dot(narrow[...], wide[...], preferred_element_type=f32)
    q_part[...] = (both[:, :128] + both[:, 128:]).reshape(16, 8, 128)
    to_genes(0, lambda at: q_part.at[at], q_gene.at[gene])
    q_gene[gene] = q_part[gene]
    pair_sum(3)
    y_ring[y] = y_pair[y]

    def lanes_of(at):
        return pl.ds(pl.multiple_of(at * 512, 512), 512)

    def project(step, carry):
        at = lax.rem(near + step, 4)
        part = jnp.dot(narrow[...], masked[:, lanes_of(at)], preferred_element_type=f32)
        for n in range(4):
            p_send[at, n] = part[:, 128 * n:128 * n + 128]
        return carry

    lax.fori_loop(0, 4, project, 0)
    for step in (2, 1, 3):
        at = lax.rem(near + step, 4)
        to_near(2, at, p_send.at[at], p_one.at[near])
    p_one[near] = p_send[near]

    low_ref[:, :128] = (loadings_ref[...] - high_ref[:, :128].astype(f32)).astype(bf16)
    arrived(q_gene.at[pl.ds(0, 15)], recv_sem.at[0])
    q_cell[cell] = jnp.sum(q_gene[...], axis=0)
    to_cells(1, lambda at: q_cell.at[cell], q_cell.at[cell])
    for step in (1, 3, 2):
        source = lax.rem(y + step, 4)
        arrived(y_ring.at[source], ring_sem.at[1, source])
    y_full[cell] = jnp.sum(y_ring[...], axis=0)
    for n, step in enumerate((2, 1, 3)):
        to = lax.rem(y + step, 4)
        copy(y_full.at[cell], y_full.at[cell], full_sem.at[0, 1 + n], full_sem.at[1, cell],
             {"cell_0": to}).start()
    copy(y_full.at[cell], y_full.at[cell], full_sem.at[0, 0], full_sem.at[1, cell], partner).start()
    arrived(q_cell.at[pl.ds(0, 7)], recv_sem.at[1])
    q_full[gene] = jnp.sum(q_cell[...], axis=0)
    to_genes(3, lambda at: q_full.at[gene], q_full.at[gene])
    arrived(three(p_one), recv_sem.at[2])
    p_mid[...] = jnp.sum(p_one[...], axis=0)
    for step in (2, 1, 3):
        at = lax.rem(far + step, 4)
        to_far(6, at, p_mid.at[at], p_two.at[far])
    p_two[far] = p_mid[far]

    arrived(q_full.at[pl.ds(0, 15)], recv_sem.at[3])
    fitted[...] = dot(loadings_ref[...], q_full[...].reshape(128, 128), 1, 0).reshape(8, rows, 128)

    def sketch_part(source):
        at = pl.ds(pl.multiple_of(source * rows, rows), rows)
        part = y_full[source] - fitted[source]
        upper = part.astype(bf16)
        lower = (part - upper.astype(f32)).astype(bf16)
        high_ref[at, 128:] = upper
        low_ref[at, 128:] = lower
        split[:128, at] = upper.T
        split[128:, at] = lower.T

    def arrive_and_split(source):
        arrived(y_full.at[source], full_sem.at[1, source])
        sketch_part(source)

    sketch_part(cell)
    arrive_and_split(2 * y + 1 - k)
    for step in (1, 3, 2):
        source = lax.rem(y + step, 4) * 2 + k
        arrived(y_full.at[source], full_sem.at[1, source])
        copy(y_full.at[source], y_full.at[source], full_sem.at[0, 3 + step],
             full_sem.at[1, source], partner).start()
        sketch_part(source)
    for step in (1, 3, 2):
        arrive_and_split(lax.rem(y + step, 4) * 2 + 1 - k)


    own = jnp.concatenate(
        [split[pl.ds(pl.multiple_of(16 * cell + h, 16), 16), :] for h in (0, 128)], axis=0
    )
    part = jnp.dot(own, high_ref[...], preferred_element_type=f32)
    part = part + jnp.dot(own, low_ref[...], preferred_element_type=f32)
    t_one[near] = part[:16] + part[16:]
    for step in (2, 1, 3):
        to_near(4, lax.rem(near + step, 4), t_one.at[near], t_one.at[near])

    def inner(at, half):
        lanes = pl.ds(pl.multiple_of(at * 512 + half * 256, 256), 256)
        part = jnp.dot(split[...], masked[:, lanes], preferred_element_type=f32)
        part = part[:128] + part[128:]
        for n in range(2):
            z_send[at, 2 * half + n] = part[:, 128 * n:128 * n + 128]

    for step in (2, 1, 3):
        at = lax.rem(near + step, 4)
        for half in range(2):
            inner(at, half)
            to_near(5, at, z_send.at[at, pl.ds(2 * half, 2)], z_one.at[near, pl.ds(2 * half, 2)])
    arrived(three(t_one), recv_sem.at[4])
    t_two[far] = jnp.sum(t_one[...], axis=0)
    for step in (2, 1, 3):
        to_far(7, lax.rem(far + step, 4), t_two.at[far], t_two.at[far])
    inner(near, 0)
    inner(near, 1)
    z_one[near] = z_send[near]
    arrived(three(t_two), recv_sem.at[7])
    t_full[cell] = jnp.sum(t_two[...], axis=0)
    to_cells(8, lambda at: t_full.at[cell], t_full.at[cell])
    arrived(three(z_one), recv_sem.at[5])
    for step in (2, 1, 3):
        at = lax.rem(far + step, 4)
        z_mid[at] = jnp.sum(z_one[:, at], axis=0)
        to_far(9, at, z_mid.at[at], z_two.at[far])
    z_two[far] = jnp.sum(z_one[:, far], axis=0)
    arrived(t_full.at[pl.ds(0, 7)], recv_sem.at[8])

    arrived(three(p_two), recv_sem.at[6])
    projection = jnp.sum(p_two[...], axis=0)
    explained = dot(t_full[...].reshape(128, 256)[:, :128], projection, 1, 0)
    c_send[:, :8] = dot(projection, projection, 1, 1).reshape(16, 8, 128)
    arrived(three(z_two), recv_sem.at[9])
    residual = jnp.sum(z_two[...], axis=0) - explained
    c_send[:, 8:16] = dot(residual, projection, 1, 1).reshape(16, 8, 128)
    c_send[:, 16:] = dot(residual, residual, 1, 1).reshape(16, 8, 128)
    to_genes(10, lambda at: c_send.at[at], c_recv.at[gene])
    c_recv[gene] = c_send[gene]
    products = t_full[...].reshape(128, 256)
    basis_ref[...] = inverse_factor(work, products[:, 128:])
    arrived(c_recv.at[pl.ds(0, 15)], recv_sem.at[10])
    c_cell[cell] = jnp.sum(c_recv[...], axis=0)
    to_cells(11, lambda at: c_cell.at[cell], c_cell.at[cell])
    arrived(c_cell.at[pl.ds(0, 7)], recv_sem.at[11])
    c_full[gene] = jnp.sum(c_cell[...], axis=0)
    to_genes(12, lambda at: c_full.at[gene], c_full.at[gene])
    arrived(c_full.at[pl.ds(0, 15)], recv_sem.at[12])
    parts = [c_full[:, 8 * n:8 * n + 8].reshape(128, 128) for n in range(3)]
    size = 128
    inverse = basis_ref[...]
    values = values_ref[...]
    mixed = dot(inverse, jnp.concatenate(parts[1:], axis=1), 1, 0)
    cross = mixed[:, :size] / cells_total
    corner = dot(mixed[:, size:], inverse, 1, 1)
    squares = jnp.broadcast_to(values * values, (size, size)) * identity(size)
    image[:, :size] = parts[0] / cells_total + squares
    image[:, size:] = cross.T
    core[...] = right_parts(
        jnp.concatenate(
            [image[...], jnp.concatenate([cross, corner / cells_total], axis=1)], axis=0
        ),
        0,
    )

    def rotation_of(last):
        return left_parts(inverse_factor(work, dot(last, last, 1, 1)), 1)

    def sweep(step, carry):
        last = image[...]
        following = right_parts(of_parts(left_parts(last, 1), core[...]), 0)
        image[...] = of_parts(rotation_of(last), following)
        return carry

    lax.fori_loop(0, SWEEPS - 1, sweep, 0)
    last = image[...]
    following = right_parts(of_parts(left_parts(last, 1), core[...]), 0)
    lifted = of_parts(left_parts(last[:, size:], 1), right_parts(basis_ref[...], 0))
    lifted = right_parts(jnp.concatenate([last[:, :size], lifted], axis=1), 0)
    last_parts = right_parts(last, 0)
    rotation = rotation_of(last)
    turn = of_parts(rotation, lifted) * genes_total**0.5
    upper = turn.astype(jnp.bfloat16)
    lower = (turn - upper.astype(jnp.float32)).astype(jnp.bfloat16)
    turns = jnp.concatenate([upper, lower], axis=0)

    def onto(left, right):
        return lax.dot_general(
            left, right, (((1,), (1,)), ((), ())), preferred_element_type=jnp.float32
        )

    both = onto(high_ref[...], turns)
    out_ref[...] = both[:, :size] + (both[:, size:] + onto(low_ref[...], upper))
    products = of_parts(rotation, last_parts) * of_parts(rotation, following)
    singular_ref[...] = jnp.sqrt(jnp.sum(products.T, axis=0, keepdims=True))

    for n in range(4):
        sent(y_pair.at[0], pair_sem.at[0, n])
    for n in range(3):
        sent(y_pair.at[0], ring_sem.at[0, n])
    for n in range(7):
        sent(y_full.at[0], full_sem.at[0, n])
    for phase, ref in ((1, q_cell), (8, t_full), (11, c_cell)):
        sent(ref.at[pl.ds(0, 7)], send_sem.at[phase])
    for phase, ref in ((0, q_gene), (3, q_full), (10, c_recv), (12, c_full)):
        sent(ref.at[pl.ds(0, 15)], send_sem.at[phase])
    for phase, ref in ((2, p_one), (4, t_one), (5, z_one), (6, p_two), (7, t_two), (9, z_two)):
        sent(three(ref), send_sem.at[phase])


def group_call(counts, loadings, test_matrix, tile_mask, values, cells_total, genes_total):
    f32, bf16 = jnp.float32, jnp.bfloat16
    genes, cells = counts.shape
    rows, share = genes // 8, cells // 16
    whole = pl.BlockSpec(memory_space=pltpu.VMEM)
    dma = pltpu.SemaphoreType.DMA
    quarter = pltpu.VMEM((4, 4, 128, share), f32)
    return pl.pallas_call(
        functools.partial(group_kernel, genes, cells_total, genes_total),
        out_shape=(
            jax.ShapeDtypeStruct((genes, 128), f32),
            jax.ShapeDtypeStruct((1, 128), f32),
        ),
        in_specs=[
            pl.BlockSpec(memory_space=pltpu.HBM),
            pl.BlockSpec(memory_space=pltpu.HBM),
            whole,
            pl.BlockSpec(memory_space=pltpu.SMEM),
            whole,
        ],
        out_specs=(whole, whole),
        scratch_shapes=[
            pltpu.VMEM((genes, 128), f32),
            pltpu.VMEM((genes, 256), bf16),
            pltpu.VMEM((genes, 256), bf16),
            pltpu.VMEM((6 * 256, 256), bf16),
            pltpu.VMEM((128, 128), f32),
            pltpu.VMEM((128, 256), f32),
            pltpu.VMEM((genes, cells), bf16),
            pltpu.VMEM((128, genes), bf16),
            pltpu.VMEM((genes, 256), bf16),
            pltpu.VMEM((256, genes), bf16),
            pltpu.VMEM((8, rows, 128), f32),
            pltpu.VMEM((128, 256), f32),
            pltpu.VMEM((8, rows, 128), f32),
            pltpu.VMEM((4, rows, 128), f32),
            pltpu.VMEM((4, rows, 128), f32),
            pltpu.VMEM((8, rows, 128), f32),
            pltpu.VMEM((16, 8, 128), f32),
            pltpu.VMEM((8, 8, 128), f32),
            pltpu.VMEM((16, 8, 128), f32),
            pltpu.VMEM((16, 8, 128), f32),
            quarter,
            quarter,
            pltpu.VMEM((4, 128, share), f32),
            pltpu.VMEM((4, 128, share), f32),
            quarter,
            quarter,
            pltpu.VMEM((4, 128, share), f32),
            pltpu.VMEM((4, 128, share), f32),
            pltpu.VMEM((4, 16, 256), f32),
            pltpu.VMEM((4, 16, 256), f32),
            pltpu.VMEM((8, 16, 256), f32),
            pltpu.VMEM((16, 24, 128), f32),
            pltpu.VMEM((16, 24, 128), f32),
            pltpu.VMEM((8, 24, 128), f32),
            pltpu.VMEM((16, 24, 128), f32),
            dma((9,)),
            dma((2, 4)),
            dma((2, 4)),
            dma((2, 8)),
            dma((13,)),
            dma((13,)),
        ],
        compiler_params=pltpu.CompilerParams(
            collective_id=0, has_side_effects=True, vmem_limit_bytes=GROUP_VMEM
        ),
        name="group",
    )(counts, loadings, test_matrix, tile_mask, values.reshape(1, -1))


def local(counts, loadings, values, test_matrix, tile_mask):
    cells_total = counts.shape[1] * lax.axis_size(CELL)
    genes_total = counts.shape[0] * lax.axis_size(GENE)
    new_loadings, singular = group_call(
        counts, loadings, test_matrix, tile_mask, values, cells_total, genes_total
    )
    return (new_loadings, singular[0])


def solution(mesh):
    torus = Mesh(mesh.devices.reshape(4, 4, 4, 2), ("gene_0", "gene_1", "cell_0", "cell_1"))
    placed = (P(GENE, CELL), P(GENE, None), P(), P(CELL, None), P(GENE, CELL))
    return jax.shard_map(
        local, mesh=torus, in_specs=placed, out_specs=(P(GENE, None), P()), check_vma=False
    )
```
